32 devices in a mesh: vocab: 8 (over z, x), dp: 4 (over y, core).
Axes of the slice: x: 2, y: 2, z: 4, core: 2. Of those that a mesh axis runs over, the one named last changes fastest.
Arguments:
- out_grads: float32 [4096, 4096], P(('vocab', 'dp')), may hold values from -6 to 6
- token_ids: int32 [4096], P(('vocab', 'dp')), may hold values from 0 to 128255, as said below
Outputs:
- table_grad: bfloat16 [128256, 4096], P('vocab', 'dp')
The draws below stay inside these ranges and needn't reach their ends.
Inputs may be any that keep to these rules, and one draw needn't show every extreme that they name: `token_ids`: call ids k * 16032 to (k + 1) * 16032 - 1 block k. The 128 tokens of one device hold at most 48 ids of any one block; one block, the same for all devices, holds exactly 48 ids of every device.
All inputs are finite; a program needn't handle non-finite values.
Results may differ from the reference program's by a relative error of at most 0.001.
Values sent between devices are 32-bit elements; how exact they have to be, the bound alone decides.
A program may use at most 192 MiB of HBM per device.

```python
import jax
import jax.numpy as jnp
from jax import lax

D = 4096
VOCAB = 128256
TOK_DEV = 128
TOKENS = 4096
N_VOCAB = 8
N_DP = 4


def draw_token_ids(key, part):
    rows_own = VOCAB // N_VOCAB
    capacity = 3 * TOK_DEV // N_VOCAB
    key_hot, key_rest = jax.random.split(jax.random.fold_in(key, 71))
    hot_block = jax.random.randint(key_hot, (), 0, N_VOCAB).astype(jnp.int32)

    def one_device(sub_key):
        key_pick, key_order, key_first, key_second = jax.random.split(sub_key, 4)
        others = (hot_block + 1 + jnp.arange((N_VOCAB - 1) * capacity, dtype=jnp.int32) // capacity) % N_VOCAB
        picked = jax.random.permutation(key_pick, others)[:TOK_DEV - capacity]
        owners = jnp.concatenate([jnp.full((capacity,), hot_block, jnp.int32), picked.astype(jnp.int32)])
        owners = jax.random.permutation(key_order, owners)
        first = jax.random.randint(key_first, (TOK_DEV,), 0, rows_own).astype(jnp.int32)
        second = jax.random.randint(key_second, (TOK_DEV,), 0, rows_own).astype(jnp.int32)
        inside = first * second // rows_own
        return (owners * rows_own + inside).astype(jnp.int32)
    device_keys = jax.random.split(key_rest, N_VOCAB * N_DP)
    return jax.vmap(one_device)(device_keys).reshape(-1).astype(jnp.int32)


def level_of(rng, shape, cuts, low, top_value):
    loudness = 1.0
    for axis_at, shards_of in cuts:
        heights = jax.random.uniform(jax.random.fold_in(jax.random.fold_in(rng, 6), axis_at), (shards_of,), jnp.float32, low / len(cuts), top_value / len(cuts))
        loudness = loudness * jnp.repeat(jnp.exp(heights), shape[axis_at] // shards_of).reshape((-1,) + (1,) * (len(shape) - 1 - axis_at))
    return loudness


def centred(rng, shape, spread, most, shards=(), kind=jnp.bfloat16):
    factor_of = level_of(rng, shape, shards, -0.22, 0.18) if shards else 1.0
    result = jax.random.normal(rng, shape, jnp.float32) * spread * factor_of
    return jnp.minimum(jnp.maximum(result, -most), most).astype(kind)


def setup_inputs(seed: int = 0) -> dict:
    streams_of = jax.random.split(jax.random.key(seed), 3)
    out_grads = centred(streams_of[0], (TOKENS, D), 1.0, 6.0, ((0, 32),), jnp.float32)
    token_ids = draw_token_ids(jax.random.fold_in(streams_of[2], 71), 0)
    return dict(out_grads=out_grads, token_ids=token_ids)


def reference(out_grads, token_ids):
    width_block = 256 if D % 256 == 0 else D
    blocks = D // width_block
    pieces = out_grads.reshape(TOKENS, blocks, width_block).transpose(1, 0, 2)

    def one_block(piece):
        summed = jax.ops.segment_sum(piece, token_ids, num_segments=VOCAB)
        return summed.astype(jnp.bfloat16)

    table = lax.map(one_block, pieces)
    return table.transpose(1, 0, 2).reshape(VOCAB, D)
```

```python
import functools

import jax
import jax.numpy as jnp
from jax import lax
from jax.experimental import pallas as pl
from jax.experimental.pallas import tpu as pltpu
from jax.sharding import PartitionSpec as P

VOCAB = 128256


def ranks_in_block(owner_of):
    positions = lax.iota(jnp.int32, owner_of.shape[1])
    earlier = (owner_of[:, :, None] == owner_of[:, None, :]) & (positions[None, None, :] < positions[None, :, None])
    return jnp.sum(earlier.astype(jnp.int32), axis=2)


def table_kernel(tile, slots_ref, rows_ref, starts_ref, data_ref, out_ref, acc):
    step = pl.program_id(0)
    base = step * tile
    acc[...] = jnp.zeros_like(acc)

    @pl.loop(starts_ref[step], starts_ref[step + 1])
    def _(at):
        row = rows_ref[at] - base
        slot = slots_ref[at]
        acc[pl.ds(row, 1), :] += data_ref[pl.ds(slot, 1), :]

    out_ref[...] = acc[...].astype(out_ref.dtype)


def build_table(data, slots, rows, starts, rows_own, tile):
    count, width = data.shape
    tiles = pl.cdiv(rows_own, tile)
    return pl.pallas_call(
        functools.partial(table_kernel, tile),
        out_shape=jax.ShapeDtypeStruct((rows_own, width), jnp.bfloat16),
        grid_spec=pltpu.PrefetchScalarGridSpec(
            num_scalar_prefetch=3,
            grid=(tiles,),
            in_specs=[pl.BlockSpec((count, width), lambda i, *_: (0, 0), pipeline_mode=pl.Buffered(1))],
            out_specs=pl.BlockSpec((tile, width), lambda i, *_: (i, 0)),
            scratch_shapes=[pltpu.VMEM((tile, width), jnp.float32)],
        ),
        compiler_params=pltpu.CompilerParams(vmem_limit_bytes=40 * 2**20),
        name="table",
    )(slots, rows, starts, data)


def order_slots(ids_all, block, rows_own, capacity, tile):
    devices = ids_all.shape[0]
    mine = (ids_all // rows_own) == block
    positions = lax.iota(jnp.int32, ids_all.shape[1])
    before = mine[:, None, :] & (positions[None, None, :] < positions[None, :, None])
    rank = jnp.sum(before.astype(jnp.int32), axis=2)
    slot_ids = lax.iota(jnp.int32, capacity)
    hit = mine[:, None, :] & (rank[:, None, :] == slot_ids[None, :, None])
    local_row = ids_all - block * rows_own
    row_at = jnp.sum(jnp.where(hit, local_row[:, None, :] + 1, 0), axis=2) - 1
    row_at = row_at.reshape(-1)
    total = devices * capacity
    slots = lax.iota(jnp.int32, total)
    key = jnp.where(row_at >= 0, row_at, rows_own) * total + slots
    place = jnp.sum((key[None, :] < key[:, None]).astype(jnp.int32), axis=1)
    sorted_key = jnp.sum(jnp.where(place[None, :] == slots[:, None], key[None, :], 0), axis=1)
    sorted_row = sorted_key // total
    sorted_slot = sorted_key - sorted_row * total
    tiles = pl.cdiv(rows_own, tile)
    bounds = jnp.minimum(lax.iota(jnp.int32, tiles + 1) * tile, rows_own)
    row_key = key // total
    starts = jnp.sum((row_key[None, :] < bounds[:, None]).astype(jnp.int32), axis=1)
    return sorted_slot, sorted_row, starts


def local(out_grads, token_ids):
    owners, dp = lax.axis_size("vocab"), lax.axis_size("dp")
    tok_count, width = out_grads.shape
    rows_own = VOCAB // owners
    capacity = 3 * tok_count // owners
    tile = 1024
    ids_all = lax.all_gather(token_ids, ("vocab", "dp"), axis=0, tiled=False)
    owner_of = token_ids // rows_own
    rank = ranks_in_block(owner_of[None])[0]
    target = owner_of * capacity + rank
    pick = (target[None, :] == lax.iota(jnp.int32, owners * capacity)[:, None]).astype(jnp.float32)
    outgoing = jnp.dot(pick, out_grads, precision=lax.Precision.HIGHEST)
    outgoing = outgoing.reshape(owners, capacity, dp, width // dp).transpose(0, 2, 1, 3)
    outgoing = outgoing.reshape(owners * dp, capacity, width // dp)
    arrived = lax.all_to_all(outgoing, ("vocab", "dp"), split_axis=0, concat_axis=0, tiled=True)
    slots, rows, starts = order_slots(ids_all, lax.axis_index("vocab"), rows_own, capacity, tile)
    data = arrived.reshape(owners * dp * capacity, width // dp)
    return build_table(data, slots, rows, starts, rows_own, tile)


def solution(mesh):
    in_specs = (P(("vocab", "dp"), None), P(("vocab", "dp")))
    out_specs = P("vocab", "dp")
    return jax.shard_map(local, mesh=mesh, in_specs=in_specs, out_specs=out_specs, check_vma=False)
```

```python
import functools

import jax
import jax.numpy as jnp
from jax import lax
from jax.experimental import pallas as pl
from jax.experimental.pallas import tpu as pltpu
from jax.sharding import PartitionSpec as P

VOCAB = 128256


def ranks_in_block(owner_of):
    positions = lax.iota(jnp.int32, owner_of.shape[1])
    earlier = (owner_of[:, :, None] == owner_of[:, None, :]) & (positions[None, None, :] < positions[None, :, None])
    return jnp.sum(earlier.astype(jnp.int32), axis=2)


def table_kernel(tile, slots_ref, rows_ref, starts_ref, data_ref, out_ref, acc):
    step = pl.program_id(0)
    base = step * tile

    @pl.when(step == 0)
    def _():
        acc[...] = jnp.zeros_like(acc)

    @pl.loop(starts_ref[step], starts_ref[step + 1])
    def _(at):
        row = rows_ref[at] - base
        slot = slots_ref[at]
        acc[pl.ds(row, 1), :] += data_ref[pl.ds(slot, 1), :]

    out_ref[...] = acc[...].astype(out_ref.dtype)

    @pl.loop(starts_ref[step], starts_ref[step + 1])
    def _(at):
        acc[pl.ds(rows_ref[at] - base, 1), :] = jnp.zeros((1, acc.shape[1]), acc.dtype)


def build_table(data, slots, rows, starts, rows_own, tile):
    count, width = data.shape
    tiles = pl.cdiv(rows_own, tile)
    return pl.pallas_call(
        functools.partial(table_kernel, tile),
        out_shape=jax.ShapeDtypeStruct((rows_own, width), jnp.bfloat16),
        grid_spec=pltpu.PrefetchScalarGridSpec(
            num_scalar_prefetch=3,
            grid=(tiles,),
            in_specs=[pl.BlockSpec((count, width), lambda i, *_: (0, 0), pipeline_mode=pl.Buffered(1))],
            out_specs=pl.BlockSpec((tile, width), lambda i, *_: (i, 0)),
            scratch_shapes=[pltpu.VMEM((tile, width), jnp.float32)],
        ),
        compiler_params=pltpu.CompilerParams(vmem_limit_bytes=40 * 2**20),
        name="table",
    )(slots, rows, starts, data)


def order_slots(ids_all, block, rows_own, capacity, tile):
    devices = ids_all.shape[0]
    mine = (ids_all // rows_own) == block
    positions = lax.iota(jnp.int32, ids_all.shape[1])
    before = mine[:, None, :] & (positions[None, None, :] < positions[None, :, None])
    rank = jnp.sum(before.astype(jnp.int32), axis=2)
    slot_ids = lax.iota(jnp.int32, capacity)
    hit = mine[:, None, :] & (rank[:, None, :] == slot_ids[None, :, None])
    local_row = ids_all - block * rows_own
    row_at = jnp.sum(jnp.where(hit, local_row[:, None, :] + 1, 0), axis=2) - 1
    row_at = row_at.reshape(-1)
    total = devices * capacity
    slots = lax.iota(jnp.int32, total)
    key = jnp.where(row_at >= 0, row_at, rows_own) * total + slots
    place = jnp.sum((key[None, :] < key[:, None]).astype(jnp.int32), axis=1)
    sorted_key = jnp.sum(jnp.where(place[None, :] == slots[:, None], key[None, :], 0), axis=1)
    sorted_row = sorted_key // total
    sorted_slot = sorted_key - sorted_row * total
    tiles = pl.cdiv(rows_own, tile)
    bounds = jnp.minimum(lax.iota(jnp.int32, tiles + 1) * tile, rows_own)
    row_key = key // total
    starts = jnp.sum((row_key[None, :] < bounds[:, None]).astype(jnp.int32), axis=1)
    return sorted_slot, sorted_row, starts


def flip(a, k, n):
    total, bit = 0, 1
    while bit < n:
        total = total + (((a // bit) % 2) + ((k // bit) % 2)) % 2 * bit
        bit *= 2
    return total


def exchange_kernel(n, dp, capacity, ids_ref, picked_ref, ids_all, arrived, sem_out, sem_in, ids_out, ids_in, own_sem):
    v, d = lax.axis_index("vocab"), lax.axis_index("dp")
    me = v * dp + d
    width = arrived.shape[1]
    others = n * dp - 1

    def piece(block, column):
        return picked_ref.at[
            pl.ds(pl.multiple_of(block * capacity, 8), capacity), pl.ds(pl.multiple_of(column * width, 128), width)
        ]

    def landing(source):
        return arrived.at[pl.ds(pl.multiple_of(source * capacity, 8), capacity)]

    own_ids = pltpu.make_async_copy(ids_ref, ids_all.at[me], own_sem.at[0])
    own_ids.start()
    own = pltpu.make_async_copy(piece(v, d), landing(me), own_sem.at[1])

    def send(i, _):
        k = others - i
        block, column = flip(v, k // dp, n), (d + k % dp) % dp
        where = dict(device_id=(block, column), device_id_type=pl.DeviceIdType.MESH)
        pltpu.make_async_remote_copy(ids_ref, ids_all.at[me], ids_out, ids_in, **where).start()
        pltpu.make_async_remote_copy(piece(block, column), landing(me), sem_out, sem_in, **where).start()
        return 0

    lax.fori_loop(0, others, send, 0)
    own.start()
    own_ids.wait()
    own.wait()
    all_ids = ids_all.at[pl.ds(0, others)]
    all_rows = arrived.at[pl.ds(0, others * capacity)]
    for sem in (ids_out, ids_in):
        pltpu.make_async_copy(all_ids, all_ids, sem).wait()
    for sem in (sem_out, sem_in):
        pltpu.make_async_copy(all_rows, all_rows, sem).wait()


def exchange(ids, picked, n, dp, capacity):
    width = picked.shape[1] // dp
    return pl.pallas_call(
        functools.partial(exchange_kernel, n, dp, capacity),
        out_shape=(
            jax.ShapeDtypeStruct((n * dp,) + ids.shape, ids.dtype),
            jax.ShapeDtypeStruct((n * dp * capacity, width), picked.dtype),
        ),
        in_specs=[pl.BlockSpec(memory_space=pl.ANY)] * 2,
        out_specs=(pl.BlockSpec(memory_space=pl.ANY),) * 2,
        scratch_shapes=[pltpu.SemaphoreType.DMA] * 4 + [pltpu.SemaphoreType.DMA((2,))],
        compiler_params=pltpu.CompilerParams(has_side_effects=True),
        name="exchange",
    )(ids, picked)


def local(out_grads, token_ids):
    owners, dp = lax.axis_size("vocab"), lax.axis_size("dp")
    tok_count, width = out_grads.shape
    rows_own = VOCAB // owners
    capacity = pl.cdiv(3 * tok_count // owners, 8) * 8
    tile = 1024
    owner_of = token_ids // rows_own
    rank = ranks_in_block(owner_of[None])[0]
    target = owner_of * capacity + rank
    pick = (target[None, :] == lax.iota(jnp.int32, owners * capacity)[:, None]).astype(jnp.float32)
    picked = jnp.dot(pick, out_grads, precision=lax.Precision.HIGHEST)
    ids_all, data = exchange(token_ids[None], picked, owners, dp, capacity)
    slots, rows, starts = order_slots(ids_all[:, 0], lax.axis_index("vocab"), rows_own, capacity, tile)
    return build_table(data, slots, rows, starts, rows_own, tile)


def solution(mesh):
    in_specs = (P(("vocab", "dp"), None), P(("vocab", "dp")))
    out_specs = P("vocab", "dp")
    return jax.shard_map(local, mesh=mesh, in_specs=in_specs, out_specs=out_specs, check_vma=False)
```

```python
import functools

import jax
import jax.numpy as jnp
from jax import lax
from jax.experimental import pallas as pl
from jax.experimental.pallas import tpu as pltpu
from jax.sharding import PartitionSpec as P

VOCAB = 128256


def ranks_in_block(owner_of):
    positions = lax.iota(jnp.int32, owner_of.shape[1])
    earlier = (owner_of[:, :, None] == owner_of[:, None, :]) & (positions[None, None, :] < positions[None, :, None])
    return jnp.sum(earlier.astype(jnp.int32), axis=2)


def table_kernel(tile, slots_ref, rows_ref, starts_ref, data_ref, out_ref, acc):
    step = pl.program_id(0)
    base = step * tile

    @pl.when(step == 0)
    def _():
        acc[...] = jnp.zeros_like(acc)

    @pl.loop(starts_ref[step], starts_ref[step + 1])
    def _(at):
        row = rows_ref[at] - base
        slot = slots_ref[at]
        acc[pl.ds(row, 1), :] += data_ref[pl.ds(slot, 1), :]

    out_ref[...] = acc[...].astype(out_ref.dtype)

    @pl.loop(starts_ref[step], starts_ref[step + 1])
    def _(at):
        acc[pl.ds(rows_ref[at] - base, 1), :] = jnp.zeros((1, acc.shape[1]), acc.dtype)


def build_table(data, slots, rows, starts, rows_own, tile):
    count, width = data.shape
    tiles = pl.cdiv(rows_own, tile)
    return pl.pallas_call(
        functools.partial(table_kernel, tile),
        out_shape=jax.ShapeDtypeStruct((rows_own, width), jnp.bfloat16),
        grid_spec=pltpu.PrefetchScalarGridSpec(
            num_scalar_prefetch=3,
            grid=(tiles,),
            in_specs=[pl.BlockSpec((count, width), lambda i, *_: (0, 0), pipeline_mode=pl.Buffered(1))],
            out_specs=pl.BlockSpec((tile, width), lambda i, *_: (i, 0)),
            scratch_shapes=[pltpu.VMEM((tile, width), jnp.float32)],
        ),
        compiler_params=pltpu.CompilerParams(vmem_limit_bytes=40 * 2**20),
        name="table",
    )(slots, rows, starts, data)


def order_slots(ids_all, block, rows_own, capacity, tile):
    devices = ids_all.shape[0]
    mine = (ids_all // rows_own) == block
    positions = lax.iota(jnp.int32, ids_all.shape[1])
    before = mine[:, None, :] & (positions[None, None, :] < positions[None, :, None])
    rank = jnp.sum(before.astype(jnp.int32), axis=2)
    slot_ids = lax.iota(jnp.int32, capacity)
    hit = mine[:, None, :] & (rank[:, None, :] == slot_ids[None, :, None])
    local_row = ids_all - block * rows_own
    row_at = jnp.sum(jnp.where(hit, local_row[:, None, :] + 1, 0), axis=2) - 1
    row_at = row_at.reshape(-1)
    total = devices * capacity
    slots = lax.iota(jnp.int32, total)
    key = jnp.where(row_at >= 0, row_at, rows_own) * total + slots
    place = jnp.sum((key[None, :] < key[:, None]).astype(jnp.int32), axis=1)
    sorted_key = jnp.sum(jnp.where(place[None, :] == slots[:, None], key[None, :], 0), axis=1)
    sorted_row = sorted_key // total
    sorted_slot = sorted_key - sorted_row * total
    tiles = pl.cdiv(rows_own, tile)
    bounds = jnp.minimum(lax.iota(jnp.int32, tiles + 1) * tile, rows_own)
    row_key = key // total
    starts = jnp.sum((row_key[None, :] < bounds[:, None]).astype(jnp.int32), axis=1)
    return sorted_slot, sorted_row, starts


def flip(a, k, n):
    total, bit = 0, 1
    while bit < n:
        total = total + (((a // bit) % 2) + ((k // bit) % 2)) % 2 * bit
        bit *= 2
    return total


def exchange_kernel(n, dp, capacity, ids_ref, picked_ref, ids_all, arrived, sem_out, sem_in, ids_out, ids_in, own_sem):
    v, d = lax.axis_index("vocab"), lax.axis_index("dp")
    me = v * dp + d
    width = arrived.shape[1]
    others = n * dp - 1

    def piece(block, column):
        return picked_ref.at[
            pl.ds(pl.multiple_of(block * capacity, 8), capacity), pl.ds(pl.multiple_of(column * width, 128), width)
        ]

    def landing(source):
        return arrived.at[pl.ds(pl.multiple_of(source * capacity, 8), capacity)]

    own_ids = pltpu.make_async_copy(ids_ref, ids_all.at[me], own_sem)
    own_ids.start()

    def send(i, _):
        k = others - i
        block, column = flip(v, k // dp, n), (d + k % dp) % dp
        where = dict(device_id=(block, column), device_id_type=pl.DeviceIdType.MESH)
        pltpu.make_async_remote_copy(ids_ref, ids_all.at[me], ids_out, ids_in, **where).start()
        pltpu.make_async_remote_copy(piece(block, column), landing(me), sem_out, sem_in, **where).start()
        return 0

    lax.fori_loop(0, others, send, 0)
    for column in range(dp):

        @pl.when(d == column)
        def _():
            landing(me)[...] = picked_ref[
                pl.ds(pl.multiple_of(v * capacity, 8), capacity), column * width : (column + 1) * width
            ]

    own_ids.wait()
    all_ids = ids_all.at[pl.ds(0, others)]
    all_rows = arrived.at[pl.ds(0, others * capacity)]
    where = dict(device_id=(flip(v, 1, n), d), device_id_type=pl.DeviceIdType.MESH)
    pltpu.make_async_remote_copy(all_ids, all_ids, ids_out, ids_in, **where).wait()
    pltpu.make_async_remote_copy(all_rows, all_rows, sem_out, sem_in, **where).wait()


def exchange(ids, picked, n, dp, capacity):
    width = picked.shape[1] // dp
    return pl.pallas_call(
        functools.partial(exchange_kernel, n, dp, capacity),
        out_shape=(
            jax.ShapeDtypeStruct((n * dp,) + ids.shape, ids.dtype),
            jax.ShapeDtypeStruct((n * dp * capacity, width), picked.dtype),
        ),
        in_specs=[pl.BlockSpec(memory_space=pl.ANY), pl.BlockSpec(memory_space=pltpu.VMEM)],
        out_specs=(pl.BlockSpec(memory_space=pl.ANY), pl.BlockSpec(memory_space=pltpu.VMEM)),
        scratch_shapes=[pltpu.SemaphoreType.DMA] * 5,
        compiler_params=pltpu.CompilerParams(has_side_effects=True, vmem_limit_bytes=40 * 2**20),
        name="exchange",
    )(ids, picked)


def local(out_grads, token_ids):
    owners, dp = lax.axis_size("vocab"), lax.axis_size("dp")
    tok_count, width = out_grads.shape
    rows_own = VOCAB // owners
    capacity = pl.cdiv(3 * tok_count // owners, 8) * 8
    tile = 1024
    owner_of = token_ids // rows_own
    rank = ranks_in_block(owner_of[None])[0]
    target = owner_of * capacity + rank
    pick = (target[None, :] == lax.iota(jnp.int32, owners * capacity)[:, None]).astype(jnp.float32)
    picked = jnp.dot(pick, out_grads, precision=lax.Precision.HIGHEST)
    ids_all, data = exchange(token_ids[None], picked, owners, dp, capacity)
    slots, rows, starts = order_slots(ids_all[:, 0], lax.axis_index("vocab"), rows_own, capacity, tile)
    return build_table(data, slots, rows, starts, rows_own, tile)


def solution(mesh):
    in_specs = (P(("vocab", "dp"), None), P(("vocab", "dp")))
    out_specs = P("vocab", "dp")
    return jax.shard_map(local, mesh=mesh, in_specs=in_specs, out_specs=out_specs, check_vma=False)
```
